16 devices in a mesh: rows: 16 (over z, y, x, core).
Axes of the slice: x: 2, y: 2, z: 2, core: 2. Of those that a mesh axis runs over, the one named last changes fastest.
Arguments:
- wave_fn: float32 [256, 4, 4, 256], P('rows')
- left_env: bfloat16 [32, 256, 256], P(None, 'rows')
- op_pair: bfloat16 [32, 16, 16], replicated
- right_env: bfloat16 [32, 256, 256], replicated
Outputs:
- output 1: float32 [7, 256, 4, 4, 256], P(None, 'rows')
- output 2: float32 [6], replicated
- output 3: float32 [6], replicated
All inputs are finite; a program needn't handle non-finite values.
Results may differ from the reference program's by a relative error of at most 0.0116381.
Values are sent between devices in bfloat16 or wider.
A program may use at most 1 GiB of HBM per device.

```python
import jax
import jax.numpy as jnp
from jax import lax

BOND_DIM = 256
PHYS_DIM = 4
NUM_TERMS = 32
NUM_STEPS = 6


def sym_noise(rng_key, num_mats, mat_size):
    raw_draw = jax.random.normal(rng_key, (num_mats, mat_size, mat_size), jnp.float32)
    return (raw_draw + jnp.swapaxes(raw_draw, 1, 2)) * (0.5 ** 0.5) * mat_size ** -0.5


def setup_inputs(seed: int = 0) -> dict:
    key_list = jax.random.split(jax.random.key(seed), 7)
    pair_dim = PHYS_DIM * PHYS_DIM
    shift_left = jax.random.uniform(key_list[0], (NUM_TERMS, 1, 1), jnp.float32, 0.3, 0.9)
    shift_pair = jax.random.uniform(key_list[1], (NUM_TERMS, 1, 1), jnp.float32, 0.3, 0.9)
    shift_right = jax.random.uniform(key_list[2], (NUM_TERMS, 1, 1), jnp.float32, 0.3, 0.9)
    left_env = sym_noise(key_list[3], NUM_TERMS, BOND_DIM) + shift_left * jnp.eye(BOND_DIM, dtype=jnp.float32)
    op_pair = (sym_noise(key_list[4], NUM_TERMS, pair_dim) + shift_pair * jnp.eye(pair_dim, dtype=jnp.float32)) * NUM_TERMS ** -0.5
    right_env = sym_noise(key_list[5], NUM_TERMS, BOND_DIM) + shift_right * jnp.eye(BOND_DIM, dtype=jnp.float32)
    wave_fn = jax.random.normal(key_list[6], (BOND_DIM, PHYS_DIM, PHYS_DIM, BOND_DIM), jnp.float32)
    return {"wave_fn": wave_fn, "left_env": left_env.astype(jnp.bfloat16), "op_pair": op_pair.astype(jnp.bfloat16), "right_env": right_env.astype(jnp.bfloat16)}


def matvec(vec_in, left_env, op_pair, right_env):
    pair_dim = PHYS_DIM * PHYS_DIM
    flat_in = vec_in.astype(jnp.bfloat16).reshape(BOND_DIM, pair_dim * BOND_DIM)

    def add_term(acc_sum, term_ops):
        left_k, pair_k, right_k = term_ops
        left_out = jnp.dot(left_k, flat_in, preferred_element_type=jnp.float32).astype(jnp.bfloat16)
        left_out = left_out.reshape(BOND_DIM, pair_dim, BOND_DIM)
        mid_out = jnp.einsum("qr,arc->aqc", pair_k.astype(jnp.float32), left_out.astype(jnp.float32)).astype(jnp.bfloat16)
        part_out = jnp.dot(mid_out.reshape(BOND_DIM * pair_dim, BOND_DIM), right_k.T, preferred_element_type=jnp.float32)
        return acc_sum + part_out, None

    start_sum = jnp.zeros((BOND_DIM * pair_dim, BOND_DIM), jnp.float32)
    sigma_all = lax.scan(add_term, start_sum, (left_env, op_pair, right_env))[0]
    return sigma_all.reshape(BOND_DIM, PHYS_DIM, PHYS_DIM, BOND_DIM)


def reference(wave_fn, left_env, op_pair, right_env):
    vec_count = BOND_DIM * BOND_DIM * PHYS_DIM * PHYS_DIM
    first_vec = wave_fn / jnp.sqrt(jnp.sum(wave_fn * wave_fn) / vec_count)

    def lanczos_step(carry_in, unused):
        prev_vec, cur_vec, beta_prev = carry_in
        sigma_all = matvec(cur_vec, left_env, op_pair, right_env)
        alpha_val = jnp.sum(sigma_all * cur_vec) / vec_count
        resid_vec = sigma_all - alpha_val * cur_vec - beta_prev * prev_vec
        beta_val = jnp.sqrt(jnp.sum(resid_vec * resid_vec) / vec_count)
        next_vec = resid_vec / beta_val
        return (cur_vec, next_vec, beta_val), (next_vec, alpha_val, beta_val)

    start_carry = (jnp.zeros_like(first_vec), first_vec, jnp.zeros((), jnp.float32))
    later_vecs, alphas, betas = lax.scan(lanczos_step, start_carry, None, length=NUM_STEPS)[1]
    return jnp.concatenate([first_vec[None], later_vecs], axis=0), alphas, betas
```

```python
import functools

import jax
import jax.numpy as jnp
from jax import lax
from jax.experimental import pallas as pl
from jax.experimental.pallas import tpu as pltpu
from jax.sharding import PartitionSpec as P

NUM_STEPS = 6
MESH = pl.DeviceIdType.MESH
NDEV = 16
PART_EDGES = ((0, 6, 11, 16), (0, 5, 11, 16))
LANES = 128


def kernel(n_count, psi_ref, left_hbm, pair_ref, right_hbm, out_hbm, alpha_ref, beta_ref,
           u_ref, left_ref, right_ref, kron_ref, x_ref, y_ref, sigma_ref, vec_ref, msg_ref, box_ref, bprev_ref,
           ici_send, ici_recv, d2d_send, d2d_recv, sc_send, sc_recv, load_sem, out_sem):
    me = lax.axis_index("rows")
    core = lax.rem(me, 2)
    bits = [lax.rem(me // (2 << d), 2) for d in range(3)]
    partner = me + 1 - 2 * core

    def flip(dev, mask):
        for d in range(3):
            if mask >> d & 1:
                dev = dev + (2 << d) * (1 - 2 * bits[d])
        return dev

    barrier = pltpu.get_barrier_semaphore()
    others = [lax.rem(me + i, NDEV) for i in range(1, NDEV)]
    for dev in others:
        pl.semaphore_signal(barrier, inc=1, device_id=(dev,), device_id_type=MESH)
    loads = [pltpu.make_async_copy(left_hbm, left_ref, load_sem.at[0])]
    for h in range(2):
        loads.append(pltpu.make_async_copy(right_hbm.at[:, h * LANES:(h + 1) * LANES, :], right_ref.at[h], load_sem.at[1 + h]))
    for ld in loads:
        ld.start()

    lane = lax.broadcasted_iota(jnp.int32, (1, LANES), 1)

    def exchange(vals):
        row = jnp.zeros((1, LANES), jnp.float32)
        for t, val in enumerate(vals):
            row = jnp.where(lane == t, val, row)
        msg_ref[...] = row
        box_ref[me] = row
        copies = []
        for i, dev in enumerate(others):
            copies.append(pltpu.make_async_remote_copy(
                src_ref=msg_ref, dst_ref=box_ref.at[me], send_sem=sc_send.at[i], recv_sem=sc_recv.at[NDEV - 2 - i],
                device_id=(dev,), device_id_type=MESH))
        for cp in copies:
            cp.start()
        for i, dev in enumerate(others):
            pltpu.make_async_remote_copy(
                src_ref=msg_ref, dst_ref=box_ref.at[dev], send_sem=sc_send.at[i], recv_sem=sc_recv.at[i],
                device_id=(dev,), device_id_type=MESH).wait_recv()
        for cp in copies:
            cp.wait_send()
        return box_ref[...].reshape(NDEV, LANES)

    def total(arr):
        part = jnp.sum(arr, axis=0)
        part = part[:, :LANES] + part[:, LANES:]
        return jnp.sum(part, axis=(0, 1), keepdims=True)

    exp_row = (lax.broadcasted_iota(jnp.int32, (128, 16), 0) // 8 == lax.broadcasted_iota(jnp.int32, (128, 16), 1)).astype(jnp.bfloat16)
    exp_col = (lax.broadcasted_iota(jnp.int32, (16, 128), 1) // 8 == lax.broadcasted_iota(jnp.int32, (16, 128), 0)).astype(jnp.bfloat16)
    diag = lax.rem(lax.broadcasted_iota(jnp.int32, (128, 128), 0), 8) == lax.rem(lax.broadcasted_iota(jnp.int32, (128, 128), 1), 8)
    wide = jnp.dot(pair_ref[...].reshape(512, 16), exp_col, preferred_element_type=jnp.float32).astype(jnp.bfloat16)
    for k in range(32):
        full = jnp.dot(exp_row, wide[k * 16:(k + 1) * 16, :], preferred_element_type=jnp.float32)
        kron_ref[k] = jnp.where(diag, full, 0.0).astype(jnp.bfloat16)

    pl.semaphore_wait(barrier, NDEV - 1)

    psi = psi_ref[...]
    got = exchange([total(psi * psi)])
    norm = jnp.sqrt(jnp.sum(got[:, 0:1], axis=0, keepdims=True) / n_count)
    vec_ref[0] = psi / norm
    vec_ref[1] = jnp.zeros_like(psi)
    bprev_ref[...] = jnp.zeros_like(bprev_ref)
    for ld in loads:
        ld.wait()

    def region(h, dev, p):
        lo, hi = PART_EDGES[h][p], PART_EDGES[h][p + 1]
        return u_ref.at[h, dev, :, lo * LANES:hi * LANES]

    def dims(p):
        return p, (p + 1) % 3, (p + 2) % 3

    def send_ici(started, h, p, mask, which):
        d = dims(p)[which]
        d0, d1, _ = dims(p)
        slot = {0: which, 1 << d0: 2 + which, 1 << d1: 5, 1 << d0 | 1 << d1: 6}[mask]
        reg = region(h, flip(me, mask), p)
        cp = pltpu.make_async_remote_copy(
            src_ref=reg, dst_ref=reg, send_sem=ici_send.at[h, p, slot], recv_sem=ici_recv.at[h, p, mask ^ (1 << d)],
            device_id=(flip(me, 1 << d),), device_id_type=MESH)
        cp.start()
        started.append(cp)

    def send_d2d(started, h, p, mask):
        reg = region(h, flip(me, mask), p)
        cp = pltpu.make_async_remote_copy(
            src_ref=reg, dst_ref=reg, send_sem=d2d_send.at[h, p, mask], recv_sem=d2d_recv.at[h, p, mask],
            device_id=(partner,), device_id_type=MESH)
        cp.start()
        started.append(cp)

    def wait_ici(h, p, mask):
        reg = region(h, flip(me, mask), p)
        pltpu.make_async_remote_copy(
            src_ref=reg, dst_ref=reg, send_sem=ici_send.at[h, p, 0], recv_sem=ici_recv.at[h, p, mask],
            device_id=(partner,), device_id_type=MESH).wait_recv()

    def wait_d2d(h, p, mask):
        reg = region(h, flip(partner, mask), p)
        pltpu.make_async_remote_copy(
            src_ref=reg, dst_ref=reg, send_sem=d2d_send.at[h, p, mask], recv_sem=d2d_recv.at[h, p, mask],
            device_id=(partner,), device_id_type=MESH).wait_recv()

    def apply_half(h):
        left = left_ref[...].reshape(512, 256)
        for rp in range(8):
            cols = u_ref[h, :, :, rp * 256:(rp + 1) * 256].reshape(256, 256)
            res = jnp.dot(left, cols, preferred_element_type=jnp.float32)
            lo = res[:, :LANES].reshape(64, 8, LANES)
            hi = res[:, LANES:].reshape(64, 8, LANES)
            x_ref[:, rp * 16:(rp + 1) * 16, :] = jnp.concatenate([lo, hi], axis=1).astype(jnp.bfloat16)
        for k in range(32):
            rhs = jnp.concatenate([x_ref[2 * k], x_ref[2 * k + 1]], axis=1)
            res = jnp.dot(kron_ref[k], rhs, preferred_element_type=jnp.float32).astype(jnp.bfloat16)
            y_ref[0:128, k * LANES:(k + 1) * LANES] = res[:, :LANES]
            y_ref[128:256, k * LANES:(k + 1) * LANES] = res[:, LANES:]
        return jnp.dot(y_ref[...], right_ref[h].reshape(4096, 256), preferred_element_type=jnp.float32).reshape(32, 8, 256)

    def out_copy(slot, j):
        return pltpu.make_async_copy(vec_ref.at[slot], out_hbm.at[j], out_sem.at[slot])

    def step(j, carry):
        cur = lax.rem(j, 2)
        prv = 1 - cur
        vec = vec_ref[cur]
        for h in range(2):
            for r in range(16):
                tile = jnp.concatenate([vec[r, :, h * LANES:(h + 1) * LANES], vec[16 + r, :, h * LANES:(h + 1) * LANES]], axis=0)
                u_ref[h, me, :, r * LANES:(r + 1) * LANES] = tile.astype(jnp.bfloat16)
        started = []
        for which in range(3):
            for p in range(3):
                send_ici(started, 0, p, 0, which)
        for p in range(3):
            send_ici(started, 1, p, 0, 0)
        for h in range(2):
            for p in range(3):
                send_d2d(started, h, p, 0)
        out_copy(cur, j).start()
        prev = vec_ref[prv]
        beta_prev = bprev_ref[0:1, 0:1]
        s_vv = total(vec * vec)
        s_pv = total(prev * vec)

        def first_hop(h):
            for p in range(3):
                m = 1 << dims(p)[0]
                wait_ici(h, p, m)
                send_ici(started, h, p, m, 1)
                send_ici(started, h, p, m, 2)
                send_d2d(started, h, p, m)

        def second_hop(h, mask_of):
            for p in range(3):
                m = mask_of(*dims(p))
                wait_ici(h, p, m)
                send_ici(started, h, p, m, 2)
                send_d2d(started, h, p, m)

        def last_hop(h, mask_of):
            for p in range(3):
                m = mask_of(*dims(p))
                wait_ici(h, p, m)
                send_d2d(started, h, p, m)

        first_hop(0)
        for which in (1, 2):
            for p in range(3):
                send_ici(started, 1, p, 0, which)
        second_hop(0, lambda a, b, c: 1 << b)
        last_hop(0, lambda a, b, c: 1 << c)
        first_hop(1)
        second_hop(0, lambda a, b, c: 1 << a | 1 << b)
        second_hop(1, lambda a, b, c: 1 << b)
        last_hop(0, lambda a, b, c: 1 << a | 1 << c)
        last_hop(0, lambda a, b, c: 1 << b | 1 << c)
        last_hop(1, lambda a, b, c: 1 << c)
        second_hop(1, lambda a, b, c: 1 << a | 1 << b)
        last_hop(0, lambda a, b, c: 7)
        for p in range(3):
            for m in range(8):
                wait_d2d(0, p, m)
        sigma_ref[...] = apply_half(0)
        last_hop(1, lambda a, b, c: 1 << a | 1 << c)
        last_hop(1, lambda a, b, c: 1 << b | 1 << c)
        last_hop(1, lambda a, b, c: 7)
        for p in range(3):
            for m in range(8):
                wait_d2d(1, p, m)
        sigma = sigma_ref[...] + apply_half(1)
        sigma_ref[...] = sigma
        for cp in started:
            cp.wait_send()

        s_sv = total(sigma * vec)
        has = s_vv > 0.0
        proj = jnp.where(has, (s_sv - beta_prev * s_pv) / jnp.where(has, s_vv, 1.0), 0.0)
        res = sigma - beta_prev * prev - proj * vec
        got = exchange([s_sv, total(res * res), total(res * vec), s_vv, proj])
        alpha = jnp.sum(got[:, 0:1], axis=0, keepdims=True) / n_count
        shift = got[:, 4:5] - alpha
        sq = got[:, 1:2] + 2.0 * (shift * got[:, 2:3]) + (shift * got[:, 3:4]) * shift
        beta = jnp.sqrt(jnp.sum(sq, axis=0, keepdims=True) / n_count)
        new = (sigma_ref[...] - alpha * vec_ref[cur] - beta_prev * vec_ref[prv]) / beta

        @pl.when(j > 0)
        def _():
            out_copy(prv, j - 1).wait()

        vec_ref[prv] = new
        bprev_ref[...] = jnp.broadcast_to(beta, bprev_ref.shape)
        alpha_ref[j] = alpha[0, 0]
        beta_ref[j] = beta[0, 0]
        return carry

    lax.fori_loop(0, NUM_STEPS, step, 0)
    last = out_copy(NUM_STEPS % 2, NUM_STEPS)
    last.start()
    out_copy((NUM_STEPS - 1) % 2, NUM_STEPS - 1).wait()
    last.wait()


def solution(mesh):
    def local_run(wave_rows, left_rows, op_pair, right_env):
        psi = wave_rows.reshape(2, 8, 16, 256).transpose(0, 2, 1, 3).reshape(32, 8, 256)
        vmem = pl.BlockSpec(memory_space=pltpu.VMEM)
        smem = pl.BlockSpec(memory_space=pltpu.SMEM)
        hbm = pl.BlockSpec(memory_space=pl.ANY)
        vecs, alpha, beta = pl.pallas_call(
            functools.partial(kernel, float(wave_rows.size * NDEV)),
            out_shape=(jax.ShapeDtypeStruct((NUM_STEPS + 1, 32, 8, 256), jnp.float32),
                       jax.ShapeDtypeStruct((NUM_STEPS,), jnp.float32),
                       jax.ShapeDtypeStruct((NUM_STEPS,), jnp.float32)),
            in_specs=[vmem, hbm, vmem, hbm],
            out_specs=(hbm, smem, smem),
            scratch_shapes=[
                pltpu.VMEM((2, NDEV, 16, 2048), jnp.bfloat16),
                pltpu.VMEM((32, 16, 256), jnp.bfloat16),
                pltpu.VMEM((2, 32, LANES, 256), jnp.bfloat16),
                pltpu.VMEM((32, 128, 128), jnp.bfloat16),
                pltpu.VMEM((64, 128, LANES), jnp.bfloat16),
                pltpu.VMEM((256, 4096), jnp.bfloat16),
                pltpu.VMEM((32, 8, 256), jnp.float32),
                pltpu.VMEM((2, 32, 8, 256), jnp.float32),
                pltpu.VMEM((1, LANES), jnp.float32),
                pltpu.VMEM((NDEV, 1, LANES), jnp.float32),
                pltpu.VMEM((8, LANES), jnp.float32),
                pltpu.SemaphoreType.DMA((2, 3, 7)),
                pltpu.SemaphoreType.DMA((2, 3, 8)),
                pltpu.SemaphoreType.DMA((2, 3, 8)),
                pltpu.SemaphoreType.DMA((2, 3, 8)),
                pltpu.SemaphoreType.DMA((NDEV - 1,)),
                pltpu.SemaphoreType.DMA((NDEV - 1,)),
                pltpu.SemaphoreType.DMA((3,)),
                pltpu.SemaphoreType.DMA((2,)),
            ],
            compiler_params=pltpu.CompilerParams(collective_id=0, has_side_effects=True, vmem_limit_bytes=48 * 1024 * 1024),
        )(psi, left_rows, op_pair, right_env)
        vecs = vecs.reshape(7, 2, 16, 8, 256).transpose(0, 1, 3, 2, 4).reshape(7, 16, 4, 4, 256)
        return vecs, alpha, beta

    return jax.shard_map(local_run, mesh=mesh, in_specs=(P("rows"), P(None, "rows"), P(), P()), out_specs=(P(None, "rows"), P(), P()), check_vma=False)
```
